32 devices in a mesh: row: 4 (over y, core), phi: 8 (over z, x).
Axes of the slice: x: 2, y: 2, z: 4, core: 2. Of those that a mesh axis runs over, the one named last changes fastest.
Arguments:
- hydro_vars: float32 [5, 128, 128, 256], P(None, 'row', 'phi'), may hold values from -6 to 6
- face_b: float32 [3, 128, 128, 256], P(None, 'row', 'phi'), may hold values from -6 to 6
- widths: int32 [16], replicated, may hold values from 2 to 128, as said below
- diffusion: float32 [5, 256], replicated, may hold values from 0.01 to 0.06
Outputs:
- conserved: float32 [8, 128, 128, 256], P(None, 'row', 'phi')
- faces_out: float32 [3, 128, 128, 256], P(None, 'row', 'phi')
The draws below stay inside these ranges and needn't reach their ends.
Inputs may be any that keep to these rules, and one draw needn't show every extreme that they name: `widths`: every width is a power of two that divides 128; the two cycles next to the poles (entries 0 and 15) use 128.
All inputs are finite; a program needn't handle non-finite values.
Results may differ from the reference program's by a relative error of at most 0.0001.
Values sent between devices are 32-bit elements; how exact they have to be, the bound alone decides.
A program may use at most 64 MiB of HBM per device.

```python
import math
import jax
import jax.numpy as jnp
from jax import lax

NTH = 256
CYCLES = 8
NR = 128
PHI_CELLS = 128


def draw_widths(key, part):
    top = PHI_CELLS.bit_length() - 1
    powers = jax.random.randint(jax.random.fold_in(key, 7), (2 * CYCLES,), 1, top + 1)
    powers = powers.at[0].set(top).at[2 * CYCLES - 1].set(top)
    return jnp.power(2, powers).astype(jnp.int32)


def block_scale(rng, extent, pieces, low, high):
    loudness, own = 1.0, jax.random.fold_in(rng, 6)
    for position, blocks in pieces:
        draws = jnp.exp(jax.random.uniform(jax.random.fold_in(own, position), (blocks,), jnp.float32, low / len(pieces), high / len(pieces)))
        loudness = loudness * jnp.repeat(draws, extent[position] // blocks).reshape([-1 if axis == position else 1 for axis in range(len(extent))])
    return loudness


def centred(rng, extent, scale, limit, cuts=(), kind=jnp.bfloat16):
    values = jax.random.normal(rng, extent, jnp.float32) * scale
    if len(cuts) > 0:
        values = block_scale(rng, extent, cuts, -0.22, 0.18) * values
    return jnp.clip(values, min=-limit, max=limit).astype(kind)


def setup_inputs(seed: int = 0) -> dict:
    key_of = jax.random.split(jax.random.key(seed), 5)
    hydro_vars = centred(key_of[0], (5, NR, PHI_CELLS, NTH), 1.0, 6.0, ((1, 4), (2, 8)), jnp.float32)
    face_b = centred(key_of[1], (3, NR, PHI_CELLS, NTH), 1.0, 6.0, ((1, 4), (2, 8)), jnp.float32)
    widths = draw_widths(jax.random.fold_in(key_of[4], 71), 0)
    diffusion = jnp.clip(jnp.exp(jax.random.uniform(key_of[3], (5, NTH), jnp.float32, math.log(0.01), math.log(0.06))), 0.01, 0.06)
    return dict(hydro_vars=hydro_vars, face_b=face_b, widths=widths, diffusion=diffusion)


def stencil(padded, axis, count):
    parts = [lax.slice_in_dim(padded, offset, offset + count, axis=axis) for offset in range(5)]
    return (16.0 * (parts[1] + parts[3]) - (parts[0] + parts[4]) - 30.0 * parts[2]) / 12.0


def fourth(values, axis, wrapped):
    count = values.shape[axis]
    pads = [(0, 0)] * values.ndim
    pads[axis] = (2, 2)
    padded = jnp.pad(values, pads, mode="wrap") if wrapped else jnp.pad(values, pads)
    return stencil(padded, axis, count)


def block_means(cycles, axis, width):
    cells = cycles.shape[axis]
    result = cycles
    for power in range(1, cells.bit_length()):
        size = 2 ** power
        shape = cycles.shape[:axis] + (cells // size, size) + cycles.shape[axis + 1:]
        means = jnp.mean(cycles.reshape(shape), axis=axis + 1, keepdims=True)
        means = jnp.broadcast_to(means, shape).reshape(cycles.shape)
        result = jnp.where(width == size, means, result)
    return result


def reference(hydro_vars, face_b, widths, diffusion):
    fields = jnp.concatenate([hydro_vars, face_b], 0)
    theta_cells = fields.shape[3]
    polar_cycles = jnp.concatenate([fields[..., :CYCLES], fields[..., theta_cells - CYCLES:]], 3)
    averaged = block_means(polar_cycles, 2, widths)
    fields = jnp.concatenate([averaged[..., :CYCLES], fields[..., CYCLES:theta_cells - CYCLES], averaged[..., CYCLES:]], 3)
    hydro = fields[:5]
    change = fourth(hydro, 1, False) + fourth(hydro, 2, True) + fourth(hydro, 3, False)
    smoothed = hydro + diffusion[:, None, None, :] * change
    radial = fields[5]
    polar_face = fields[6]
    azimuth = fields[7]
    radial_next = jnp.concatenate([radial[1:], jnp.zeros_like(radial[:1])], 0)
    polar_next = jnp.concatenate([polar_face[..., 1:], jnp.zeros_like(polar_face[..., :1])], 2)
    azimuth_next = jnp.roll(azimuth, -1, axis=1)
    cell_field = 0.5 * jnp.stack([radial + radial_next, polar_face + polar_next, azimuth + azimuth_next])
    return jnp.concatenate([smoothed, cell_field], 0), fields[5:]
```

```python
import functools

import jax
import jax.numpy as jnp
from jax import lax
from jax.experimental import pallas as pl
from jax.experimental.pallas import tpu as pltpu
from jax.sharding import PartitionSpec as P

MESH = pl.DeviceIdType.MESH
LANES = 128
EARLY = 2


def kernel(
    nrow, nphi, rows, cells, cycles,
    widths, hydro, face, diffusion, conserved, faces_out,
    H, F, O, SL, SR, PL, PR, SF, RF, FN, M, MG, ELO, EHI, EL, ER,
    load_sem, out_sem, send_phi, recv_phi, send_mean, recv_mean, send_row, recv_row,
):
    nvar = hydro.shape[0]
    nface = face.shape[0]
    theta = hydro.shape[2]
    tiles = theta // LANES
    last = tiles - 1
    body = rows * cells
    row = lax.axis_index("row")
    phi = lax.axis_index("phi")
    left = lax.rem(phi + nphi - 1, nphi)
    right = lax.rem(phi + 1, nphi)
    packed = 2 * cycles

    loads = []
    for k in range(nvar):
        loads.append([pltpu.make_async_copy(
            hydro.at[k, :, pl.ds(t * LANES, LANES)], H.at[k, t, pl.ds(2 * cells, body)], load_sem.at[k, t])
            for t in range(tiles)])
    for k in range(nface):
        loads.append([pltpu.make_async_copy(
            face.at[k, :, pl.ds(t * LANES, LANES)], F.at[k, t], load_sem.at[nvar + k, t])
            for t in range(tiles)])
    for group in loads:
        for c in group:
            c.start()

    barrier = pltpu.get_barrier_semaphore()
    for step in range(1, nphi):
        pl.semaphore_signal(barrier, inc=1, device_id={"phi": lax.rem(phi + step, nphi)}, device_id_type=MESH)

    @pl.when(row > 0)
    def _():
        pl.semaphore_signal(barrier, inc=1, device_id={"row": row - 1}, device_id_type=MESH)

    @pl.when(row < nrow - 1)
    def _():
        pl.semaphore_signal(barrier, inc=1, device_id={"row": row + 1}, device_id_type=MESH)

    lane = lax.broadcasted_iota(jnp.int32, (1, LANES), 1)
    width_raw = jnp.zeros((1, LANES), jnp.int32)
    width_packed = jnp.zeros((1, LANES), jnp.int32)
    slot = lax.rem(lane, packed)
    for j in range(cycles):
        width_raw = jnp.where(lane == j, widths[j], width_raw)
        width_raw = jnp.where(lane == LANES - cycles + j, widths[cycles + j], width_raw)
        width_packed = jnp.where(slot == cycles + j, widths[j], width_packed)
        width_packed = jnp.where(slot == j, widths[cycles + j], width_packed)
    low = lane < cycles
    high = lane >= LANES - cycles

    def part(t):
        return slice(t * LANES, (t + 1) * LANES)

    def pack(value, f):
        return pltpu.roll(value, (cycles + packed * f) % LANES, 1)

    def unpack(value, f):
        return pltpu.roll(value, (-(cycles + packed * f)) % LANES, 1)

    def layer(ref, k, first, cell, t):
        return ref[k, t, pl.ds(first + cell, rows, stride=cells), :]

    def phi_copies(k):
        return (
            pltpu.make_async_remote_copy(
                src_ref=SL.at[k], dst_ref=PR.at[k], send_sem=send_phi.at[0, k], recv_sem=recv_phi.at[0, k],
                device_id={"phi": left}, device_id_type=MESH),
            pltpu.make_async_remote_copy(
                src_ref=SR.at[k], dst_ref=PL.at[k], send_sem=send_phi.at[1, k], recv_sem=recv_phi.at[1, k],
                device_id={"phi": right}, device_id_type=MESH),
        )

    def pack_halo(k):
        for t in range(tiles):
            for i in range(2):
                SL[k, i, :, part(t)] = layer(H, k, 2 * cells, i, t)
                SR[k, i, :, part(t)] = layer(H, k, 2 * cells, cells - 2 + i, t)

    for k in range(EARLY):
        for c in loads[k]:
            c.wait()
        pack_halo(k)

    peers = nphi - 1 + jnp.where(row > 0, 1, 0) + jnp.where(row < nrow - 1, 1, 0)
    pl.semaphore_wait(barrier, peers)
    for k in range(EARLY):
        for c in phi_copies(k):
            c.start()
    for k in range(EARLY, nvar + nface):
        for c in loads[k]:
            c.wait()

    for t in range(tiles):
        SF[:, part(t)] = layer(F, nface - 1, 0, 0, t)
    for k in range(EARLY, nvar):
        pack_halo(k)

    index = lax.broadcasted_iota(jnp.int32, (cells, LANES), 0)

    def local_average(r, carry):
        mean_row = jnp.zeros((1, LANES), jnp.float32)
        lo_row = jnp.zeros((1, LANES), jnp.float32)
        hi_row = jnp.zeros((1, LANES), jnp.float32)
        for f in range(nvar + nface):
            ref, k, base = (H, f, 2 * cells) if f < nvar else (F, f - nvar, 0)
            where = pl.ds(pl.multiple_of(base + r * cells, cells), cells)
            first = ref[k, 0, where, :]
            final = ref[k, last, where, :]
            total = jnp.where(low, first, final)
            result = total
            size = 1
            while size < cells:
                forward = pltpu.roll(total, cells - size, 0)
                if 2 * size < cells:
                    backward = pltpu.roll(total, size, 0)
                    forward = jnp.where((index & size) == 0, forward, backward)
                total = total + forward
                size *= 2
                result = jnp.where(width_raw == size, total * (1.0 / size), result)
            ref[k, 0, where, :] = jnp.where(low, result, first)
            second = result if last > 0 else jnp.where(low, result, final)
            keep = final if last > 0 else second
            ref[k, last, where, :] = jnp.where(high, result, keep)
            mine = (lane >= packed * f) & (lane < packed * (f + 1))
            mean_row = jnp.where(mine, pack(total[0:1] * (1.0 / cells), f), mean_row)
            lo_row = jnp.where(mine, pack(result[0:1], f), lo_row)
            hi_row = jnp.where(mine, pack(result[cells - 1 : cells], f), hi_row)
        M[pl.ds(r, 1), :] = mean_row
        ELO[pl.ds(r, 1), :] = lo_row
        EHI[pl.ds(r, 1), :] = hi_row
        return carry

    lax.fori_loop(0, rows, local_average, 0)

    def mean_copy(step):
        return pltpu.make_async_remote_copy(
            src_ref=M, dst_ref=MG.at[phi], send_sem=send_mean.at[step], recv_sem=recv_mean.at[step],
            device_id={"phi": lax.rem(phi + step, nphi)}, device_id_type=MESH)

    edge_left = pltpu.make_async_remote_copy(
        src_ref=ELO, dst_ref=ER, send_sem=send_phi.at[0, nvar], recv_sem=recv_phi.at[0, nvar],
        device_id={"phi": left}, device_id_type=MESH)
    edge_right = pltpu.make_async_remote_copy(
        src_ref=EHI, dst_ref=EL, send_sem=send_phi.at[1, nvar], recv_sem=recv_phi.at[1, nvar],
        device_id={"phi": right}, device_id_type=MESH)
    face_left = pltpu.make_async_remote_copy(
        src_ref=SF, dst_ref=RF, send_sem=send_phi.at[0, nvar + 1], recv_sem=recv_phi.at[0, nvar + 1],
        device_id={"phi": left}, device_id_type=MESH)
    for step in range(1, nphi):
        mean_copy(step).start()
    edge_left.start()
    edge_right.start()
    for k in range(EARLY, nvar):
        for c in phi_copies(k):
            c.start()
    face_left.start()

    MG[phi] = M[...]
    for step in range(1, nphi):
        mean_copy(step).wait_recv()

    def group_mean(who, initial):
        result = initial
        size = 2
        while size <= nphi:
            start = (who // size) * size
            total = MG[start]
            for i in range(1, size):
                total = total + MG[start + i]
            result = jnp.where(width_packed == size * cells, total * (1.0 / size), result)
            size *= 2
        return result

    M2 = group_mean(phi, M[...])
    ELO_next = group_mean(right, jnp.zeros_like(M2))
    EHI_next = group_mean(left, jnp.zeros_like(M2))
    MG[phi] = M2
    wide = width_raw > cells
    low_wide = low & wide
    high_wide = high & wide

    def wide_average(r):
        mean_row = MG[phi, pl.ds(r, 1), :]
        for f in range(nvar + nface):
            ref, k, base = (H, f, 2 * cells) if f < nvar else (F, f - nvar, 0)
            where = pl.ds(pl.multiple_of(base + r * cells, cells), cells)
            mean = jnp.broadcast_to(unpack(mean_row, f), (cells, LANES))
            ref[k, 0, where, :] = jnp.where(low_wide, mean, ref[k, 0, where, :])
            ref[k, last, where, :] = jnp.where(high_wide, mean, ref[k, last, where, :])

    for r in (0, 1, rows - 2, rows - 1):
        wide_average(r)

    lax.fori_loop(2, rows - 2, lambda r, c: (wide_average(r), c)[1], 0)

    down = pltpu.make_async_remote_copy(
        src_ref=H.at[:, :, pl.ds(2 * cells, 2 * cells)], dst_ref=H.at[:, :, pl.ds((rows + 2) * cells, 2 * cells)],
        send_sem=send_row.at[0], recv_sem=recv_row.at[0], device_id={"row": row - 1}, device_id_type=MESH)
    down_face = pltpu.make_async_remote_copy(
        src_ref=F.at[0, :, pl.ds(0, cells)], dst_ref=FN,
        send_sem=send_row.at[1], recv_sem=recv_row.at[1], device_id={"row": row - 1}, device_id_type=MESH)
    up = pltpu.make_async_remote_copy(
        src_ref=H.at[:, :, pl.ds(rows * cells, 2 * cells)], dst_ref=H.at[:, :, pl.ds(0, 2 * cells)],
        send_sem=send_row.at[2], recv_sem=recv_row.at[2], device_id={"row": row + 1}, device_id_type=MESH)

    @pl.when(row > 0)
    def _():
        down.start()
        down_face.start()

    @pl.when(row < nrow - 1)
    def _():
        up.start()

    faces_copies = [
        pltpu.make_async_copy(F.at[k, t], faces_out.at[k, :, pl.ds(t * LANES, LANES)], out_sem.at[nvar + nface + k, t])
        for k in range(nface) for t in range(tiles)]
    for c in faces_copies:
        c.start()

    @pl.when(row == 0)
    def _():
        H[:, :, pl.ds(0, 2 * cells), :] = jnp.zeros((nvar, tiles, 2 * cells, LANES), jnp.float32)

    @pl.when(row == nrow - 1)
    def _():
        H[:, :, pl.ds((rows + 2) * cells, 2 * cells), :] = jnp.zeros((nvar, tiles, 2 * cells, LANES), jnp.float32)
        FN[...] = jnp.zeros_like(FN)

    @pl.when(row > 0)
    def _():
        up.wait_recv()

    @pl.when(row < nrow - 1)
    def _():
        down.wait_recv()
        down_face.wait_recv()

    def shifted(parts, amount):
        out = []
        turned = [pltpu.roll(p, (-amount) % LANES, 1) for p in parts]
        for t in range(tiles):
            if amount > 0:
                inside = lane < LANES - amount
                other = turned[t + 1] if t + 1 < tiles else 0.0
            else:
                inside = lane >= -amount
                other = turned[t - 1] if t > 0 else 0.0
            out.append(jnp.where(inside, turned[t], other))
        return out

    def smooth_row(r, carry):
        for k in range(nvar):
            def at(offset, t):
                return H[k, t, pl.ds(pl.multiple_of((r + 2 + offset) * cells, cells), cells), :]
            mid = [at(0, t) for t in range(tiles)]
            one = [a + b for a, b in zip(shifted(mid, 1), shifted(mid, -1))]
            two = [a + b for a, b in zip(shifted(mid, 2), shifted(mid, -2))]
            for t in range(tiles):
                v = mid[t]
                s1 = one[t] + (pltpu.roll(v, 1, 0) + pltpu.roll(v, cells - 1, 0)) + (at(-1, t) + at(1, t))
                s2 = two[t] + (pltpu.roll(v, 2, 0) + pltpu.roll(v, cells - 2, 0)) + (at(-2, t) + at(2, t))
                change = (16.0 * s1 - s2 - 90.0 * v) * (1.0 / 12.0)
                O[k, t, pl.ds(pl.multiple_of(r * cells, cells), cells), :] = v + diffusion[k : k + 1, part(t)] * change
        return carry

    def field_row(r, following):
        here = pl.ds(pl.multiple_of(r * cells, cells), cells)
        polar = [F[1, t, here, :] for t in range(tiles)]
        polar_next = shifted(polar, 1)
        for t in range(tiles):
            O[nvar, t, here, :] = 0.5 * (F[0, t, here, :] + following(t))
            O[nvar + 1, t, here, :] = 0.5 * (polar[t] + polar_next[t])
            azimuth = F[2, t, here, :]
            O[nvar + 2, t, here, :] = 0.5 * (azimuth + pltpu.roll(azimuth, cells - 1, 0))

    def field_loop(r, carry):
        field_row(r, lambda t: F[0, t, pl.ds(pl.multiple_of((r + 1) * cells, cells), cells), :])
        return carry

    lax.fori_loop(0, rows - 1, field_loop, 0)
    field_row(rows - 1, lambda t: FN[t])
    outs = [[
        pltpu.make_async_copy(O.at[k, t], conserved.at[k, :, pl.ds(t * LANES, LANES)], out_sem.at[k, t])
        for t in range(tiles)] for k in range(nvar + nface)]

    def store(k):
        for c in outs[k]:
            c.start()

    store(nvar)
    store(nvar + 1)
    lax.fori_loop(0, rows, smooth_row, 0)

    edge_left.wait_recv()
    edge_right.wait_recv()
    local = width_packed <= cells
    from_left = jnp.where(local, EL[...], EHI_next)
    from_right = jnp.where(local, ER[...], ELO_next)

    def fixed(raw, edge, t):
        if t == 0:
            raw = jnp.where(low, edge, raw)
        if t == last:
            raw = jnp.where(high, edge, raw)
        return raw

    for k in range(nvar):
        for c in phi_copies(k):
            c.wait_recv()
        edge_l = unpack(from_left, k)
        edge_r = unpack(from_right, k)
        for t in range(tiles):
            scale = diffusion[k : k + 1, part(t)] * (1.0 / 12.0)
            l1 = fixed(PL[k, 1, :, part(t)], edge_l, t) - layer(H, k, 2 * cells, cells - 1, t)
            l2 = fixed(PL[k, 0, :, part(t)], edge_l, t) - layer(H, k, 2 * cells, cells - 2, t)
            r1 = fixed(PR[k, 0, :, part(t)], edge_r, t) - layer(H, k, 2 * cells, 0, t)
            r2 = fixed(PR[k, 1, :, part(t)], edge_r, t) - layer(H, k, 2 * cells, 1, t)
            for cell, term in ((0, 16.0 * l1 - l2), (1, -l1), (cells - 2, -r1), (cells - 1, 16.0 * r1 - r2)):
                spot = pl.ds(cell, rows, stride=cells)
                O[k, t, spot, :] = O[k, t, spot, :] + scale * term
        store(k)

    face_left.wait_recv()
    edge_f = unpack(from_right, nvar + nface - 1)
    for t in range(tiles):
        spot = pl.ds(cells - 1, rows, stride=cells)
        O[nvar + 2, t, spot, :] = 0.5 * (layer(F, nface - 1, 0, cells - 1, t) + fixed(RF[:, part(t)], edge_f, t))
    store(nvar + 2)

    for k in range(nvar):
        for c in phi_copies(k):
            c.wait_send()
    edge_left.wait_send()
    edge_right.wait_send()
    face_left.wait_send()
    for step in range(1, nphi):
        mean_copy(step).wait_send()

    @pl.when(row > 0)
    def _():
        down.wait_send()
        down_face.wait_send()

    @pl.when(row < nrow - 1)
    def _():
        up.wait_send()

    for c in faces_copies:
        c.wait()
    for group in outs:
        for c in group:
            c.wait()


def body(nrow, nphi, hydro_vars, face_b, widths, diffusion):
    nvar, rows, cells, theta = hydro_vars.shape
    nface = face_b.shape[0]
    cycles = widths.shape[0] // 2
    f32 = jnp.float32
    tiles = theta // LANES
    shape = lambda *s: pltpu.VMEM(s, f32)
    anywhere = pl.BlockSpec(memory_space=pl.ANY)
    conserved, faces = pl.pallas_call(
        functools.partial(kernel, nrow, nphi, rows, cells, cycles),
        out_shape=(
            jax.ShapeDtypeStruct((nvar + nface, rows * cells, theta), f32),
            jax.ShapeDtypeStruct((nface, rows * cells, theta), f32),
        ),
        in_specs=[
            pl.BlockSpec(memory_space=pltpu.SMEM),
            anywhere,
            anywhere,
            pl.BlockSpec(memory_space=pltpu.VMEM),
        ],
        out_specs=(anywhere, anywhere),
        scratch_shapes=[
            shape(nvar, tiles, (rows + 4) * cells, LANES),
            shape(nface, tiles, rows * cells, LANES),
            shape(nvar + nface, tiles, rows * cells, LANES),
            shape(nvar, 2, rows, theta),
            shape(nvar, 2, rows, theta),
            shape(nvar, 2, rows, theta),
            shape(nvar, 2, rows, theta),
            shape(rows, theta),
            shape(rows, theta),
            shape(tiles, cells, LANES),
            shape(rows, LANES),
            shape(nphi, rows, LANES),
            shape(rows, LANES),
            shape(rows, LANES),
            shape(rows, LANES),
            shape(rows, LANES),
            pltpu.SemaphoreType.DMA((nvar + nface, tiles)),
            pltpu.SemaphoreType.DMA((nvar + 2 * nface, tiles)),
            pltpu.SemaphoreType.DMA((2, nvar + 2)),
            pltpu.SemaphoreType.DMA((2, nvar + 2)),
            pltpu.SemaphoreType.DMA((nphi,)),
            pltpu.SemaphoreType.DMA((nphi,)),
            pltpu.SemaphoreType.DMA((3,)),
            pltpu.SemaphoreType.DMA((3,)),
        ],
        compiler_params=pltpu.CompilerParams(
            collective_id=0, has_side_effects=True, vmem_limit_bytes=40 * 1024 * 1024
        ),
        name="step",
    )(
        widths,
        hydro_vars.reshape(nvar, rows * cells, theta),
        face_b.reshape(nface, rows * cells, theta),
        diffusion,
    )
    return (
        conserved.reshape(nvar + nface, rows, cells, theta),
        faces.reshape(nface, rows, cells, theta),
    )


def solution(mesh):
    spec = P(None, "row", "phi", None)
    return jax.shard_map(
        functools.partial(body, mesh.shape["row"], mesh.shape["phi"]),
        mesh=mesh,
        in_specs=(spec, spec, P(), P()),
        out_specs=(spec, spec),
        check_vma=False,
    )
```

```python
import functools

import jax
import jax.numpy as jnp
from jax import lax
from jax.experimental import pallas as pl
from jax.experimental.pallas import tpu as pltpu
from jax.sharding import PartitionSpec as P

MESH = pl.DeviceIdType.MESH
LANES = 128
SUB = 8
EARLY = 1
LIMIT = 67000000


def kernel(
    nrow, nphi, rows, cells, tiles, cycles,
    widths_far, hydro, face, diffusion_far, O, F,
    H, SL, SR, PL, PR, SF, RF, FN, Q, M, MG, ELO, EHI, EL, ER,
    widths, diffusion, small_sem, load_sem, send_phi, recv_phi, send_mean, recv_mean, send_row, recv_row,
):
    nvar = hydro.shape[0]
    nface = face.shape[0]
    fields = nvar + nface
    last = tiles - 1
    blocks = cells // SUB
    ring = cells * tiles
    row = lax.axis_index("row")
    phi = lax.axis_index("phi")
    left = lax.rem(phi + nphi - 1, nphi)
    right = lax.rem(phi + 1, nphi)
    packed = 2 * cycles

    loads = [pltpu.make_async_copy(hydro.at[k], H.at[k, pl.ds(2 * ring, rows * ring)], load_sem.at[k]) for k in range(nvar)]
    loads += [pltpu.make_async_copy(face.at[k], F.at[k], load_sem.at[nvar + k]) for k in range(nface)]
    small = [
        pltpu.make_async_copy(widths_far, widths, small_sem.at[0]),
        pltpu.make_async_copy(diffusion_far, diffusion, small_sem.at[1]),
    ]
    for c in small + loads:
        c.start()

    barrier = pltpu.get_barrier_semaphore()
    for step in range(1, nphi):
        pl.semaphore_signal(barrier, inc=1, device_id={"phi": lax.rem(phi + step, nphi)}, device_id_type=MESH)

    @pl.when(row > 0)
    def _():
        pl.semaphore_signal(barrier, inc=1, device_id={"row": row - 1}, device_id_type=MESH)

    @pl.when(row < nrow - 1)
    def _():
        pl.semaphore_signal(barrier, inc=1, device_id={"row": row + 1}, device_id_type=MESH)

    for c in small:
        c.wait()
    lane = lax.broadcasted_iota(jnp.int32, (1, LANES), 1)
    width = jnp.zeros((1, LANES), jnp.int32)
    slot = lax.rem(lane, packed)
    for j in range(cycles):
        width = jnp.where(slot == cycles + j, widths[j], width)
        width = jnp.where(slot == j, widths[cycles + j], width)
    low = lane < cycles
    high = lane >= LANES - cycles
    mine = [(lane >= packed * f) & (lane < packed * (f + 1)) for f in range(fields)]

    def part(t):
        return slice(t * LANES, (t + 1) * LANES)

    def pack(value, f):
        return pltpu.roll(value, (cycles + packed * f) % LANES, 1)

    def unpack(value, f):
        return pltpu.roll(value, (-(cycles + packed * f)) % LANES, 1)

    def spot(r, b, t):
        start = r * ring + (b * tiles + t) * SUB
        return pl.ds(start if isinstance(r, int) else pl.multiple_of(start, SUB), SUB)

    def layer(r, cell, t):
        return pl.ds(r * ring + (cell // SUB * tiles + t) * SUB + cell % SUB, rows, stride=ring)

    def place(f):
        return (H, f, 2) if f < nvar else (F, f - nvar, 0)

    def phi_copies(k):
        return (
            pltpu.make_async_remote_copy(
                src_ref=SL.at[k], dst_ref=PR.at[k], send_sem=send_phi.at[0, k], recv_sem=recv_phi.at[0, k],
                device_id={"phi": left}, device_id_type=MESH),
            pltpu.make_async_remote_copy(
                src_ref=SR.at[k], dst_ref=PL.at[k], send_sem=send_phi.at[1, k], recv_sem=recv_phi.at[1, k],
                device_id={"phi": right}, device_id_type=MESH),
        )

    def pack_halo(k):
        for t in range(tiles):
            for i in range(2):
                SL[k, i, t] = H[k, layer(2, i, t), :]
                SR[k, i, t] = H[k, layer(2, cells - 2 + i, t), :]

    for k in range(EARLY):
        loads[k].wait()
        pack_halo(k)
    peers = nphi - 1 + jnp.where(row > 0, 1, 0) + jnp.where(row < nrow - 1, 1, 0)
    pl.semaphore_wait(barrier, peers)
    for k in range(EARLY):
        for c in phi_copies(k):
            c.start()
    for k in range(EARLY, fields):
        loads[k].wait()

    index = lax.broadcasted_iota(jnp.int32, (SUB, LANES), 0)

    def local_average(r, carry):
        totals = []
        for b in range(blocks):
            value = jnp.zeros((SUB, LANES), jnp.float32)
            for f in range(fields):
                ref, k, base = place(f)
                polar = jnp.where(low, ref[k, spot(r + base, b, 0), :], ref[k, spot(r + base, b, last), :])
                value = jnp.where(mine[f], pack(polar, f), value)
            totals.append(value)
        results = list(totals)
        size = 1
        while size < cells:
            if size < SUB:
                turned = []
                for v in totals:
                    forward = pltpu.roll(v, SUB - size, 0)
                    if 2 * size < SUB:
                        forward = jnp.where((index & size) == 0, forward, pltpu.roll(v, size, 0))
                    turned.append(v + forward)
                totals = turned
            else:
                hop = size // SUB
                totals = [totals[b] + totals[b ^ hop] for b in range(blocks)]
            size *= 2
            results = [jnp.where(width == size, v * (1.0 / size), old) for v, old in zip(totals, results)]
        for b in range(blocks):
            Q[pl.ds(pl.multiple_of(r * cells + b * SUB, SUB), SUB), :] = results[b]
        M[pl.ds(r, 1), :] = totals[0][0:1] * (1.0 / cells)
        ELO[pl.ds(r, 1), :] = results[0][0:1]
        EHI[pl.ds(r, 1), :] = results[blocks - 1][SUB - 1 : SUB]
        return carry

    lax.fori_loop(0, rows, local_average, 0)

    def mean_copy(step):
        return pltpu.make_async_remote_copy(
            src_ref=M, dst_ref=MG.at[phi], send_sem=send_mean.at[step], recv_sem=recv_mean.at[step],
            device_id={"phi": lax.rem(phi + step, nphi)}, device_id_type=MESH)

    edge_left = pltpu.make_async_remote_copy(
        src_ref=ELO, dst_ref=ER, send_sem=send_phi.at[0, nvar], recv_sem=recv_phi.at[0, nvar],
        device_id={"phi": left}, device_id_type=MESH)
    edge_right = pltpu.make_async_remote_copy(
        src_ref=EHI, dst_ref=EL, send_sem=send_phi.at[1, nvar], recv_sem=recv_phi.at[1, nvar],
        device_id={"phi": right}, device_id_type=MESH)
    face_left = pltpu.make_async_remote_copy(
        src_ref=SF, dst_ref=RF, send_sem=send_phi.at[0, nvar + 1], recv_sem=recv_phi.at[0, nvar + 1],
        device_id={"phi": left}, device_id_type=MESH)
    for step in range(1, nphi):
        mean_copy(step).start()
    edge_left.start()
    edge_right.start()
    for t in range(tiles):
        SF[t] = F[nface - 1, layer(0, 0, t), :]
    for k in range(EARLY, nvar):
        pack_halo(k)
    for k in range(EARLY, nvar):
        for c in phi_copies(k):
            c.start()
    face_left.start()

    MG[phi] = M[...]
    for step in range(1, nphi):
        mean_copy(step).wait_recv()

    def group_mean(who, initial):
        result = initial
        size = 2
        while size <= nphi:
            start = (who // size) * size
            total = MG[start]
            for i in range(1, size):
                total = total + MG[start + i]
            result = jnp.where(width == size * cells, total * (1.0 / size), result)
            size *= 2
        return result

    own_mean = group_mean(phi, M[...])
    next_lo = group_mean(right, jnp.zeros_like(own_mean))
    next_hi = group_mean(left, jnp.zeros_like(own_mean))
    MG[phi] = own_mean
    wide = width > cells

    def spread(r):
        mean = jnp.broadcast_to(MG[phi, pl.ds(r, 1), :], (SUB, LANES))
        for b in range(blocks):
            where = pl.ds(r * cells + b * SUB if isinstance(r, int) else pl.multiple_of(r * cells + b * SUB, SUB), SUB)
            value = jnp.where(wide, mean, Q[where, :])
            for f in range(fields):
                ref, k, base = place(f)
                polar = unpack(value, f)
                ref[k, spot(r + base, b, 0), :] = jnp.where(low, polar, ref[k, spot(r + base, b, 0), :])
                ref[k, spot(r + base, b, last), :] = jnp.where(high, polar, ref[k, spot(r + base, b, last), :])

    for r in (0, 1, rows - 2, rows - 1):
        spread(r)
    lax.fori_loop(2, rows - 2, lambda r, c: (spread(r), c)[1], 0)

    down = pltpu.make_async_remote_copy(
        src_ref=H.at[:, pl.ds(2 * ring, 2 * ring)], dst_ref=H.at[:, pl.ds((rows + 2) * ring, 2 * ring)],
        send_sem=send_row.at[0], recv_sem=recv_row.at[0], device_id={"row": row - 1}, device_id_type=MESH)
    down_face = pltpu.make_async_remote_copy(
        src_ref=F.at[0, pl.ds(0, ring)], dst_ref=FN,
        send_sem=send_row.at[1], recv_sem=recv_row.at[1], device_id={"row": row - 1}, device_id_type=MESH)
    up = pltpu.make_async_remote_copy(
        src_ref=H.at[:, pl.ds(rows * ring, 2 * ring)], dst_ref=H.at[:, pl.ds(0, 2 * ring)],
        send_sem=send_row.at[2], recv_sem=recv_row.at[2], device_id={"row": row + 1}, device_id_type=MESH)

    @pl.when(row > 0)
    def _():
        down.start()
        down_face.start()

    @pl.when(row < nrow - 1)
    def _():
        up.start()

    @pl.when(row == 0)
    def _():
        H[:, pl.ds(0, 2 * ring), :] = jnp.zeros((nvar, 2 * ring, LANES), jnp.float32)

    @pl.when(row == nrow - 1)
    def _():
        H[:, pl.ds((rows + 2) * ring, 2 * ring), :] = jnp.zeros((nvar, 2 * ring, LANES), jnp.float32)
        FN[...] = jnp.zeros_like(FN)

    def whole(ref, k, r, t):
        return jnp.concatenate([ref[k, spot(r, b, t), :] for b in range(blocks)], 0)

    def write(k, r, t, value):
        for b in range(blocks):
            O[k, spot(r, b, t), :] = value[b * SUB : (b + 1) * SUB]

    def shifted(parts, amount):
        out = []
        turned = [pltpu.roll(p, (-amount) % LANES, 1) for p in parts]
        for t in range(tiles):
            if amount > 0:
                inside = lane < LANES - amount
                other = turned[t + 1] if t + 1 < tiles else 0.0
            else:
                inside = lane >= -amount
                other = turned[t - 1] if t > 0 else 0.0
            out.append(jnp.where(inside, turned[t], other))
        return out

    def smooth_row(r):
        for k in range(nvar):
            mid = [whole(H, k, r + 2, t) for t in range(tiles)]
            one = [a + b for a, b in zip(shifted(mid, 1), shifted(mid, -1))]
            two = [a + b for a, b in zip(shifted(mid, 2), shifted(mid, -2))]
            for t in range(tiles):
                v = mid[t]
                s1 = one[t] + (pltpu.roll(v, 1, 0) + pltpu.roll(v, cells - 1, 0)) + (whole(H, k, r + 1, t) + whole(H, k, r + 3, t))
                s2 = two[t] + (pltpu.roll(v, 2, 0) + pltpu.roll(v, cells - 2, 0)) + (whole(H, k, r, t) + whole(H, k, r + 4, t))
                change = (16.0 * s1 - s2 - 90.0 * v) * (1.0 / 12.0)
                write(k, r, t, v + diffusion[k : k + 1, part(t)] * change)

    def field_row(r, following):
        polar = [whole(F, 1, r, t) for t in range(tiles)]
        polar_next = shifted(polar, 1)
        for t in range(tiles):
            write(nvar, r, t, 0.5 * (whole(F, 0, r, t) + following(t)))
            write(nvar + 1, r, t, 0.5 * (polar[t] + polar_next[t]))
            azimuth = whole(F, 2, r, t)
            write(nvar + 2, r, t, 0.5 * (azimuth + pltpu.roll(azimuth, cells - 1, 0)))

    def inner_row(r, carry):
        field_row(r, lambda t: whole(F, 0, r + 1, t))
        smooth_row(r)
        return carry

    lax.fori_loop(2, rows - 2, inner_row, 0)
    for r in (0, 1, rows - 2):
        field_row(r, lambda t, r=r: whole(F, 0, r + 1, t))

    @pl.when(row > 0)
    def _():
        up.wait_recv()

    @pl.when(row < nrow - 1)
    def _():
        down.wait_recv()
        down_face.wait_recv()

    field_row(rows - 1, lambda t: jnp.concatenate([FN[spot(0, b, t), :] for b in range(blocks)], 0))
    for r in (0, 1, rows - 2, rows - 1):
        smooth_row(r)

    edge_left.wait_recv()
    edge_right.wait_recv()
    local = width <= cells
    from_left = jnp.where(local, EL[...], next_hi)
    from_right = jnp.where(local, ER[...], next_lo)

    def fixed(raw, edge, t):
        if t == 0:
            raw = jnp.where(low, edge, raw)
        if t == last:
            raw = jnp.where(high, edge, raw)
        return raw

    for k in range(nvar):
        for c in phi_copies(k):
            c.wait_recv()
        edge_l = unpack(from_left, k)
        edge_r = unpack(from_right, k)
        for t in range(tiles):
            scale = diffusion[k : k + 1, part(t)] * (1.0 / 12.0)
            l1 = fixed(PL[k, 1, t], edge_l, t) - H[k, layer(2, cells - 1, t), :]
            l2 = fixed(PL[k, 0, t], edge_l, t) - H[k, layer(2, cells - 2, t), :]
            r1 = fixed(PR[k, 0, t], edge_r, t) - H[k, layer(2, 0, t), :]
            r2 = fixed(PR[k, 1, t], edge_r, t) - H[k, layer(2, 1, t), :]
            for cell, term in ((0, 16.0 * l1 - l2), (1, -l1), (cells - 2, -r1), (cells - 1, 16.0 * r1 - r2)):
                O[k, layer(0, cell, t), :] = O[k, layer(0, cell, t), :] + scale * term

    face_left.wait_recv()
    edge_f = unpack(from_right, fields - 1)
    for t in range(tiles):
        O[fields - 1, layer(0, cells - 1, t), :] = 0.5 * (F[nface - 1, layer(0, cells - 1, t), :] + fixed(RF[t], edge_f, t))

    for k in range(nvar):
        for c in phi_copies(k):
            c.wait_send()
    edge_left.wait_send()
    edge_right.wait_send()
    face_left.wait_send()
    for step in range(1, nphi):
        mean_copy(step).wait_send()

    @pl.when(row > 0)
    def _():
        down.wait_send()
        down_face.wait_send()

    @pl.when(row < nrow - 1)
    def _():
        up.wait_send()


def blocked(x):
    n, rows, cells, theta = x.shape
    x = x.reshape(n, rows, cells // SUB, SUB, theta // LANES, LANES)
    return x.transpose(0, 1, 2, 4, 3, 5).reshape(n, rows * cells * (theta // LANES), LANES)


def unblocked(x, rows, cells, theta):
    x = x.reshape(x.shape[0], rows, cells // SUB, theta // LANES, SUB, LANES)
    return x.transpose(0, 1, 2, 4, 3, 5).reshape(x.shape[0], rows, cells, theta)


def body(nrow, nphi, hydro_vars, face_b, widths, diffusion):
    nvar, rows, cells, theta = hydro_vars.shape
    nface = face_b.shape[0]
    fields = nvar + nface
    cycles = widths.shape[0] // 2
    tiles = theta // LANES
    ring = cells * tiles
    f32 = jnp.float32
    shape = lambda *s: pltpu.VMEM(s, f32)
    far = pl.BlockSpec(memory_space=pltpu.HBM)
    near = pl.BlockSpec(memory_space=pltpu.VMEM)
    result_bytes = (fields + nface) * rows * ring * LANES * 4
    conserved, faces = pl.pallas_call(
        functools.partial(kernel, nrow, nphi, rows, cells, tiles, cycles),
        out_shape=(
            jax.ShapeDtypeStruct((fields, rows * ring, LANES), f32),
            jax.ShapeDtypeStruct((nface, rows * ring, LANES), f32),
        ),
        in_specs=[far, far, far, far],
        out_specs=(near, near),
        scratch_shapes=[
            shape(nvar, (rows + 4) * ring, LANES),
            shape(nvar, 2, tiles, rows, LANES),
            shape(nvar, 2, tiles, rows, LANES),
            shape(nvar, 2, tiles, rows, LANES),
            shape(nvar, 2, tiles, rows, LANES),
            shape(tiles, rows, LANES),
            shape(tiles, rows, LANES),
            shape(ring, LANES),
            shape(rows * cells, LANES),
            shape(rows, LANES),
            shape(nphi, rows, LANES),
            shape(rows, LANES),
            shape(rows, LANES),
            shape(rows, LANES),
            shape(rows, LANES),
            pltpu.SMEM((2 * cycles,), jnp.int32),
            shape(nvar, theta),
            pltpu.SemaphoreType.DMA((2,)),
            pltpu.SemaphoreType.DMA((fields,)),
            pltpu.SemaphoreType.DMA((2, nvar + 2)),
            pltpu.SemaphoreType.DMA((2, nvar + 2)),
            pltpu.SemaphoreType.DMA((nphi,)),
            pltpu.SemaphoreType.DMA((nphi,)),
            pltpu.SemaphoreType.DMA((3,)),
            pltpu.SemaphoreType.DMA((3,)),
        ],
        compiler_params=pltpu.CompilerParams(
            collective_id=0, has_side_effects=True, vmem_limit_bytes=LIMIT - result_bytes
        ),
        name="step",
    )(widths, blocked(hydro_vars), blocked(face_b), diffusion)
    return unblocked(conserved, rows, cells, theta), unblocked(faces, rows, cells, theta)


def solution(mesh):
    spec = P(None, "row", "phi", None)
    return jax.shard_map(
        functools.partial(body, mesh.shape["row"], mesh.shape["phi"]),
        mesh=mesh,
        in_specs=(spec, spec, P(), P()),
        out_specs=(spec, spec),
        check_vma=False,
    )
```

```python
import functools

import jax
import jax.numpy as jnp
from jax import lax
from jax.experimental import pallas as pl
from jax.experimental.pallas import tpu as pltpu
from jax.sharding import PartitionSpec as P

MESH = pl.DeviceIdType.MESH
LANES = 128
SUB = 8
EARLY = 2
LIMIT = 58000000


def kernel(
    nrow, nphi, rows, cells, tiles, cycles,
    widths_far, hydro, face, diffusion_far, O, F,
    H, SL, SR, PL, PR, SF, RF, FN, Q, M, MG, ELO, EHI, EL, ER,
    widths, diffusion, small_sem, load_sem, send_phi, recv_phi, send_mean, recv_mean, send_row, recv_row,
):
    nvar = hydro.shape[0]
    nface = face.shape[0]
    fields = nvar + nface
    last = tiles - 1
    blocks = cells // SUB
    ring = cells * tiles
    row = lax.axis_index("row")
    phi = lax.axis_index("phi")
    left = lax.rem(phi + nphi - 1, nphi)
    right = lax.rem(phi + 1, nphi)
    packed = 2 * cycles

    loads = [pltpu.make_async_copy(hydro.at[k], H.at[k, pl.ds(2 * ring, rows * ring)], load_sem.at[k]) for k in range(nvar)]
    loads += [pltpu.make_async_copy(face.at[k], F.at[k], load_sem.at[nvar + k]) for k in range(nface)]
    small = [
        pltpu.make_async_copy(widths_far, widths, small_sem.at[0]),
        pltpu.make_async_copy(diffusion_far, diffusion, small_sem.at[1]),
    ]
    for c in small + loads:
        c.start()

    barrier = pltpu.get_barrier_semaphore()
    for step in range(1, nphi):
        pl.semaphore_signal(barrier, inc=1, device_id={"phi": lax.rem(phi + step, nphi)}, device_id_type=MESH)

    @pl.when(row > 0)
    def _():
        pl.semaphore_signal(barrier, inc=1, device_id={"row": row - 1}, device_id_type=MESH)

    @pl.when(row < nrow - 1)
    def _():
        pl.semaphore_signal(barrier, inc=1, device_id={"row": row + 1}, device_id_type=MESH)

    for c in small:
        c.wait()
    lane = lax.broadcasted_iota(jnp.int32, (1, LANES), 1)
    width = jnp.zeros((1, LANES), jnp.int32)
    slot = lax.rem(lane, packed)
    for j in range(cycles):
        width = jnp.where(slot == cycles + j, widths[j], width)
        width = jnp.where(slot == j, widths[cycles + j], width)
    low = lane < cycles
    high = lane >= LANES - cycles
    mine = [(lane >= packed * f) & (lane < packed * (f + 1)) for f in range(fields)]

    def part(t):
        return slice(t * LANES, (t + 1) * LANES)

    def pack(value, f):
        return pltpu.roll(value, (cycles + packed * f) % LANES, 1)

    def unpack(value, f):
        return pltpu.roll(value, (-(cycles + packed * f)) % LANES, 1)

    def spot(r, b, t):
        start = r * ring + (b * tiles + t) * SUB
        return pl.ds(start if isinstance(r, int) else pl.multiple_of(start, SUB), SUB)

    def layer(r, cell, t):
        return pl.ds(r * ring + (cell // SUB * tiles + t) * SUB + cell % SUB, rows, stride=ring)

    def place(f):
        return (H, f, 2) if f < nvar else (F, f - nvar, 0)

    def phi_copies(k):
        return (
            pltpu.make_async_remote_copy(
                src_ref=SL.at[k], dst_ref=PR.at[k], send_sem=send_phi.at[0, k], recv_sem=recv_phi.at[0, k],
                device_id={"phi": left}, device_id_type=MESH),
            pltpu.make_async_remote_copy(
                src_ref=SR.at[k], dst_ref=PL.at[k], send_sem=send_phi.at[1, k], recv_sem=recv_phi.at[1, k],
                device_id={"phi": right}, device_id_type=MESH),
        )

    def mean_copy(step):
        return pltpu.make_async_remote_copy(
            src_ref=M, dst_ref=MG.at[phi], send_sem=send_mean.at[step], recv_sem=recv_mean.at[step],
            device_id={"phi": lax.rem(phi + step, nphi)}, device_id_type=MESH)

    def pack_halo(k):
        for t in range(tiles):
            for i in range(2):
                SL[k, i, t] = H[k, layer(2, i, t), :]
                SR[k, i, t] = H[k, layer(2, cells - 2 + i, t), :]

    for c in loads:
        c.wait()

    def polar_cells(r, b):
        value = jnp.zeros((SUB, LANES), jnp.float32)
        for f in range(fields):
            ref, k, base = place(f)
            polar = jnp.where(low, ref[k, spot(r + base, b, 0), :], ref[k, spot(r + base, b, last), :])
            value = jnp.where(mine[f], pack(polar, f), value)
        return value

    def cell_mean(r, carry):
        value = jnp.zeros((SUB, LANES), jnp.float32)
        for f in range(fields):
            ref, k, base = place(f)
            sums = [ref[k, spot(r + base, 0, t), :] for t in (0, last)]
            for b in range(1, blocks):
                sums = [x + ref[k, spot(r + base, b, t), :] for x, t in zip(sums, (0, last))]
            value = jnp.where(mine[f], pack(jnp.where(low, sums[0], sums[1]), f), value)
        size = SUB // 2
        while size:
            value = value + pltpu.roll(value, size, 0)
            size //= 2
        M[pl.ds(r, 1), :] = value[0:1] * (1.0 / cells)
        return carry

    lax.fori_loop(0, rows, cell_mean, 0, unroll=2)
    peers = nphi - 1 + jnp.where(row > 0, 1, 0) + jnp.where(row < nrow - 1, 1, 0)
    pl.semaphore_wait(barrier, peers)
    for step in range(1, nphi):
        mean_copy(step).start()
    for k in range(EARLY):
        pack_halo(k)
        for c in phi_copies(k):
            c.start()

    index = lax.broadcasted_iota(jnp.int32, (SUB, LANES), 0)

    def local_average(r, carry):
        totals = [polar_cells(r, b) for b in range(blocks)]
        results = list(totals)
        size = 1
        while size < cells:
            if size < SUB:
                turned = []
                for v in totals:
                    forward = pltpu.roll(v, SUB - size, 0)
                    if 2 * size < SUB:
                        forward = jnp.where((index & size) == 0, forward, pltpu.roll(v, size, 0))
                    turned.append(v + forward)
                totals = turned
            else:
                hop = size // SUB
                totals = [totals[b] + totals[b ^ hop] for b in range(blocks)]
            size *= 2
            results = [jnp.where(width == size, v * (1.0 / size), old) for v, old in zip(totals, results)]
        for b in range(blocks):
            Q[pl.ds(pl.multiple_of(r * cells + b * SUB, SUB), SUB), :] = results[b]
        ELO[pl.ds(r, 1), :] = results[0][0:1]
        EHI[pl.ds(r, 1), :] = results[blocks - 1][SUB - 1 : SUB]
        return carry

    lax.fori_loop(0, rows, local_average, 0, unroll=2)

    edge_left = pltpu.make_async_remote_copy(
        src_ref=ELO, dst_ref=ER, send_sem=send_phi.at[0, nvar], recv_sem=recv_phi.at[0, nvar],
        device_id={"phi": left}, device_id_type=MESH)
    edge_right = pltpu.make_async_remote_copy(
        src_ref=EHI, dst_ref=EL, send_sem=send_phi.at[1, nvar], recv_sem=recv_phi.at[1, nvar],
        device_id={"phi": right}, device_id_type=MESH)
    face_left = pltpu.make_async_remote_copy(
        src_ref=SF, dst_ref=RF, send_sem=send_phi.at[0, nvar + 1], recv_sem=recv_phi.at[0, nvar + 1],
        device_id={"phi": left}, device_id_type=MESH)
    edge_left.start()
    edge_right.start()
    for t in range(tiles):
        SF[t] = F[nface - 1, layer(0, 0, t), :]
    for k in range(EARLY, nvar):
        pack_halo(k)
    for k in range(EARLY, nvar):
        for c in phi_copies(k):
            c.start()
    face_left.start()

    MG[phi] = M[...]
    for step in range(1, nphi):
        mean_copy(step).wait_recv()

    def group_mean(who, initial):
        result = initial
        size = 2
        while size <= nphi:
            start = (who // size) * size
            total = MG[start]
            for i in range(1, size):
                total = total + MG[start + i]
            result = jnp.where(width == size * cells, total * (1.0 / size), result)
            size *= 2
        return result

    own_mean = group_mean(phi, M[...])
    next_lo = group_mean(right, jnp.zeros_like(own_mean))
    next_hi = group_mean(left, jnp.zeros_like(own_mean))
    MG[phi] = own_mean
    wide = width > cells

    def spread(r):
        mean = jnp.broadcast_to(MG[phi, pl.ds(r, 1), :], (SUB, LANES))
        for b in range(blocks):
            where = pl.ds(r * cells + b * SUB if isinstance(r, int) else pl.multiple_of(r * cells + b * SUB, SUB), SUB)
            value = jnp.where(wide, mean, Q[where, :])
            for f in range(fields):
                ref, k, base = place(f)
                polar = unpack(value, f)
                ref[k, spot(r + base, b, 0), :] = jnp.where(low, polar, ref[k, spot(r + base, b, 0), :])
                ref[k, spot(r + base, b, last), :] = jnp.where(high, polar, ref[k, spot(r + base, b, last), :])

    for r in (0, 1, rows - 2, rows - 1):
        spread(r)
    lax.fori_loop(2, rows - 2, lambda r, c: (spread(r), c)[1], 0, unroll=2)

    down = pltpu.make_async_remote_copy(
        src_ref=H.at[:, pl.ds(2 * ring, 2 * ring)], dst_ref=H.at[:, pl.ds((rows + 2) * ring, 2 * ring)],
        send_sem=send_row.at[0], recv_sem=recv_row.at[0], device_id={"row": row - 1}, device_id_type=MESH)
    down_face = pltpu.make_async_remote_copy(
        src_ref=F.at[0, pl.ds(0, ring)], dst_ref=FN,
        send_sem=send_row.at[1], recv_sem=recv_row.at[1], device_id={"row": row - 1}, device_id_type=MESH)
    up = pltpu.make_async_remote_copy(
        src_ref=H.at[:, pl.ds(rows * ring, 2 * ring)], dst_ref=H.at[:, pl.ds(0, 2 * ring)],
        send_sem=send_row.at[2], recv_sem=recv_row.at[2], device_id={"row": row + 1}, device_id_type=MESH)

    @pl.when(row > 0)
    def _():
        down.start()
        down_face.start()

    @pl.when(row < nrow - 1)
    def _():
        up.start()

    @pl.when(row == 0)
    def _():
        H[:, pl.ds(0, 2 * ring), :] = jnp.zeros((nvar, 2 * ring, LANES), jnp.float32)

    @pl.when(row == nrow - 1)
    def _():
        H[:, pl.ds((rows + 2) * ring, 2 * ring), :] = jnp.zeros((nvar, 2 * ring, LANES), jnp.float32)
        FN[...] = jnp.zeros_like(FN)

    def whole(ref, k, r, t):
        return jnp.concatenate([ref[k, spot(r, b, t), :] for b in range(blocks)], 0)

    def write(k, r, t, value):
        for b in range(blocks):
            O[k, spot(r, b, t), :] = value[b * SUB : (b + 1) * SUB]

    def shifted(parts, amount):
        out = []
        turned = [pltpu.roll(p, (-amount) % LANES, 1) for p in parts]
        for t in range(tiles):
            if amount > 0:
                inside = lane < LANES - amount
                other = turned[t + 1] if t + 1 < tiles else 0.0
            else:
                inside = lane >= -amount
                other = turned[t - 1] if t > 0 else 0.0
            out.append(jnp.where(inside, turned[t], other))
        return out

    def smooth_row(r):
        for k in range(nvar):
            mid = [whole(H, k, r + 2, t) for t in range(tiles)]
            one = [a + b for a, b in zip(shifted(mid, 1), shifted(mid, -1))]
            two = [a + b for a, b in zip(shifted(mid, 2), shifted(mid, -2))]
            for t in range(tiles):
                v = mid[t]
                s1 = one[t] + (pltpu.roll(v, 1, 0) + pltpu.roll(v, cells - 1, 0)) + (whole(H, k, r + 1, t) + whole(H, k, r + 3, t))
                s2 = two[t] + (pltpu.roll(v, 2, 0) + pltpu.roll(v, cells - 2, 0)) + (whole(H, k, r, t) + whole(H, k, r + 4, t))
                change = (16.0 * s1 - s2 - 90.0 * v) * (1.0 / 12.0)
                write(k, r, t, v + diffusion[k : k + 1, part(t)] * change)

    def field_row(r, following):
        polar = [whole(F, 1, r, t) for t in range(tiles)]
        polar_next = shifted(polar, 1)
        for t in range(tiles):
            write(nvar, r, t, 0.5 * (whole(F, 0, r, t) + following(t)))
            write(nvar + 1, r, t, 0.5 * (polar[t] + polar_next[t]))
            azimuth = whole(F, 2, r, t)
            write(nvar + 2, r, t, 0.5 * (azimuth + pltpu.roll(azimuth, cells - 1, 0)))

    def inner_row(r, carry):
        field_row(r, lambda t: whole(F, 0, r + 1, t))
        smooth_row(r)
        return carry

    lax.fori_loop(2, rows - 2, inner_row, 0)
    for r in (0, 1, rows - 2):
        field_row(r, lambda t, r=r: whole(F, 0, r + 1, t))

    @pl.when(row > 0)
    def _():
        up.wait_recv()

    @pl.when(row < nrow - 1)
    def _():
        down.wait_recv()
        down_face.wait_recv()

    field_row(rows - 1, lambda t: jnp.concatenate([FN[spot(0, b, t), :] for b in range(blocks)], 0))
    for r in (0, 1, rows - 2, rows - 1):
        smooth_row(r)

    edge_left.wait_recv()
    edge_right.wait_recv()
    local = width <= cells
    from_left = jnp.where(local, EL[...], next_hi)
    from_right = jnp.where(local, ER[...], next_lo)

    def fixed(raw, edge, t):
        if t == 0:
            raw = jnp.where(low, edge, raw)
        if t == last:
            raw = jnp.where(high, edge, raw)
        return raw

    for k in range(nvar):
        for c in phi_copies(k):
            c.wait_recv()
        edge_l = unpack(from_left, k)
        edge_r = unpack(from_right, k)
        for t in range(tiles):
            scale = diffusion[k : k + 1, part(t)] * (1.0 / 12.0)
            l1 = fixed(PL[k, 1, t], edge_l, t) - H[k, layer(2, cells - 1, t), :]
            l2 = fixed(PL[k, 0, t], edge_l, t) - H[k, layer(2, cells - 2, t), :]
            r1 = fixed(PR[k, 0, t], edge_r, t) - H[k, layer(2, 0, t), :]
            r2 = fixed(PR[k, 1, t], edge_r, t) - H[k, layer(2, 1, t), :]
            for cell, term in ((0, 16.0 * l1 - l2), (1, -l1), (cells - 2, -r1), (cells - 1, 16.0 * r1 - r2)):
                O[k, layer(0, cell, t), :] = O[k, layer(0, cell, t), :] + scale * term

    face_left.wait_recv()
    edge_f = unpack(from_right, fields - 1)
    for t in range(tiles):
        O[fields - 1, layer(0, cells - 1, t), :] = 0.5 * (F[nface - 1, layer(0, cells - 1, t), :] + fixed(RF[t], edge_f, t))

    for k in range(nvar):
        for c in phi_copies(k):
            c.wait_send()
    edge_left.wait_send()
    edge_right.wait_send()
    face_left.wait_send()
    for step in range(1, nphi):
        mean_copy(step).wait_send()

    @pl.when(row > 0)
    def _():
        down.wait_send()
        down_face.wait_send()

    @pl.when(row < nrow - 1)
    def _():
        up.wait_send()


def spill(pieces, conserved, faces, conserved_out, faces_out, sem):
    fields = conserved.shape[0]
    size = conserved.shape[1] // pieces
    copies = []
    for k in range(fields + faces.shape[0]):
        source, target, i = (conserved, conserved_out, k) if k < fields else (faces, faces_out, k - fields)
        for p in range(pieces):
            where = pl.ds(p * size, size)
            copies.append(pltpu.make_async_copy(source.at[i, where], target.at[i, where], sem.at[k, p]))
    for c in copies:
        c.start()
    for c in copies:
        c.wait()


def blocked(x):
    n, rows, cells, theta = x.shape
    x = x.reshape(n, rows, cells // SUB, SUB, theta // LANES, LANES)
    return x.transpose(0, 1, 2, 4, 3, 5).reshape(n, rows * cells * (theta // LANES), LANES)


def unblocked(x, rows, cells, theta):
    x = x.reshape(x.shape[0], rows, cells // SUB, theta // LANES, SUB, LANES)
    return x.transpose(0, 1, 2, 4, 3, 5).reshape(x.shape[0], rows, cells, theta)


def body(nrow, nphi, hydro_vars, face_b, widths, diffusion):
    nvar, rows, cells, theta = hydro_vars.shape
    nface = face_b.shape[0]
    fields = nvar + nface
    cycles = widths.shape[0] // 2
    tiles = theta // LANES
    ring = cells * tiles
    f32 = jnp.float32
    shape = lambda *s: pltpu.VMEM(s, f32)
    far = pl.BlockSpec(memory_space=pltpu.HBM)
    near = pl.BlockSpec(memory_space=pltpu.VMEM)
    result_bytes = (fields + nface) * rows * ring * LANES * 4
    conserved, faces = pl.pallas_call(
        functools.partial(kernel, nrow, nphi, rows, cells, tiles, cycles),
        out_shape=(
            pltpu.VMEM((fields, rows * ring, LANES), f32),
            pltpu.VMEM((nface, rows * ring, LANES), f32),
        ),
        in_specs=[far, far, far, far],
        out_specs=(near, near),
        scratch_shapes=[
            shape(nvar, (rows + 4) * ring, LANES),
            shape(nvar, 2, tiles, rows, LANES),
            shape(nvar, 2, tiles, rows, LANES),
            shape(nvar, 2, tiles, rows, LANES),
            shape(nvar, 2, tiles, rows, LANES),
            shape(tiles, rows, LANES),
            shape(tiles, rows, LANES),
            shape(ring, LANES),
            shape(rows * cells, LANES),
            shape(rows, LANES),
            shape(nphi, rows, LANES),
            shape(rows, LANES),
            shape(rows, LANES),
            shape(rows, LANES),
            shape(rows, LANES),
            pltpu.SMEM((2 * cycles,), jnp.int32),
            shape(nvar, theta),
            pltpu.SemaphoreType.DMA((2,)),
            pltpu.SemaphoreType.DMA((fields,)),
            pltpu.SemaphoreType.DMA((2, nvar + 2)),
            pltpu.SemaphoreType.DMA((2, nvar + 2)),
            pltpu.SemaphoreType.DMA((nphi,)),
            pltpu.SemaphoreType.DMA((nphi,)),
            pltpu.SemaphoreType.DMA((3,)),
            pltpu.SemaphoreType.DMA((3,)),
        ],
        compiler_params=pltpu.CompilerParams(
            collective_id=0, has_side_effects=True, vmem_limit_bytes=LIMIT - result_bytes
        ),
        name="step",
    )(widths, blocked(hydro_vars), blocked(face_b), diffusion)
    pieces = 2
    conserved, faces = pl.pallas_call(
        functools.partial(spill, pieces),
        out_shape=(
            jax.ShapeDtypeStruct((fields, rows * ring, LANES), f32),
            jax.ShapeDtypeStruct((nface, rows * ring, LANES), f32),
        ),
        in_specs=[near, near],
        out_specs=(far, far),
        scratch_shapes=[pltpu.SemaphoreType.DMA((fields + nface, pieces))],
        compiler_params=pltpu.CompilerParams(vmem_limit_bytes=1000000),
        name="spill",
    )(conserved, faces)
    return unblocked(conserved, rows, cells, theta), unblocked(faces, rows, cells, theta)


def solution(mesh):
    spec = P(None, "row", "phi", None)
    return jax.shard_map(
        functools.partial(body, mesh.shape["row"], mesh.shape["phi"]),
        mesh=mesh,
        in_specs=(spec, spec, P(), P()),
        out_specs=(spec, spec),
        check_vma=False,
    )
```

```python
import functools

import jax
import jax.numpy as jnp
from jax import lax
from jax.experimental import pallas as pl
from jax.experimental.pallas import tpu as pltpu
from jax.sharding import PartitionSpec as P

MESH = pl.DeviceIdType.MESH
LANES = 128
SUB = 8
EARLY = 2
LIMIT = 58000000


def kernel(
    nrow, nphi, rows, cells, tiles, cycles,
    widths_far, hydro, face, diffusion_far, O, F,
    H, SL, SR, PL, PR, SF, RF, FN, Q, M, MG, ELO, EHI, EL, ER,
    widths, diffusion, small_sem, load_sem, send_phi, recv_phi, send_mean, recv_mean, send_row, recv_row,
):
    nvar = hydro.shape[0]
    nface = face.shape[0]
    fields = nvar + nface
    last = tiles - 1
    blocks = cells // SUB
    ring = cells * tiles
    row = lax.axis_index("row")
    phi = lax.axis_index("phi")
    left = lax.rem(phi + nphi - 1, nphi)
    right = lax.rem(phi + 1, nphi)
    packed = 2 * cycles

    loads = [pltpu.make_async_copy(hydro.at[k], H.at[k, pl.ds(2 * ring, rows * ring)], load_sem.at[k]) for k in range(nvar)]
    loads += [pltpu.make_async_copy(face.at[k], F.at[k], load_sem.at[nvar + k]) for k in range(nface)]
    small = [
        pltpu.make_async_copy(widths_far, widths, small_sem.at[0]),
        pltpu.make_async_copy(diffusion_far, diffusion, small_sem.at[1]),
    ]
    for c in small + loads:
        c.start()

    barrier = pltpu.get_barrier_semaphore()
    for step in range(1, nphi):
        pl.semaphore_signal(barrier, inc=1, device_id={"phi": lax.rem(phi + step, nphi)}, device_id_type=MESH)

    @pl.when(row > 0)
    def _():
        pl.semaphore_signal(barrier, inc=1, device_id={"row": row - 1}, device_id_type=MESH)

    @pl.when(row < nrow - 1)
    def _():
        pl.semaphore_signal(barrier, inc=1, device_id={"row": row + 1}, device_id_type=MESH)

    for c in small:
        c.wait()
    lane = lax.broadcasted_iota(jnp.int32, (1, LANES), 1)
    width = jnp.zeros((1, LANES), jnp.int32)
    slot = lax.rem(lane, packed)
    for j in range(cycles):
        width = jnp.where(slot == cycles + j, widths[j], width)
        width = jnp.where(slot == j, widths[cycles + j], width)
    low = lane < cycles
    high = lane >= LANES - cycles
    mine = [(lane >= packed * f) & (lane < packed * (f + 1)) for f in range(fields)]

    def part(t):
        return slice(t * LANES, (t + 1) * LANES)

    def pack(value, f):
        return pltpu.roll(value, (cycles + packed * f) % LANES, 1)

    def unpack(value, f):
        return pltpu.roll(value, (-(cycles + packed * f)) % LANES, 1)

    def spot(r, b, t):
        start = r * ring + (b * tiles + t) * SUB
        return pl.ds(start if isinstance(r, int) else pl.multiple_of(start, SUB), SUB)

    def layer(r, cell, t):
        return pl.ds(r * ring + (cell // SUB * tiles + t) * SUB + cell % SUB, rows, stride=ring)

    def place(f):
        return (H, f, 2) if f < nvar else (F, f - nvar, 0)

    def phi_copies(k):
        return (
            pltpu.make_async_remote_copy(
                src_ref=SL.at[k], dst_ref=PR.at[k], send_sem=send_phi.at[0, k], recv_sem=recv_phi.at[0, k],
                device_id={"phi": left}, device_id_type=MESH),
            pltpu.make_async_remote_copy(
                src_ref=SR.at[k], dst_ref=PL.at[k], send_sem=send_phi.at[1, k], recv_sem=recv_phi.at[1, k],
                device_id={"phi": right}, device_id_type=MESH),
        )

    def mean_copy(step):
        return pltpu.make_async_remote_copy(
            src_ref=M, dst_ref=MG.at[phi], send_sem=send_mean.at[step], recv_sem=recv_mean.at[step],
            device_id={"phi": lax.rem(phi + step, nphi)}, device_id_type=MESH)

    def pack_halo(k):
        for t in range(tiles):
            for i in range(2):
                SL[k, i, t] = H[k, layer(2, i, t), :]
                SR[k, i, t] = H[k, layer(2, cells - 2 + i, t), :]

    for c in loads:
        c.wait()

    def polar_cells(r, b):
        value = jnp.zeros((SUB, LANES), jnp.float32)
        for f in range(fields):
            ref, k, base = place(f)
            polar = jnp.where(low, ref[k, spot(r + base, b, 0), :], ref[k, spot(r + base, b, last), :])
            value = jnp.where(mine[f], pack(polar, f), value)
        return value

    def cell_mean(r, carry):
        value = jnp.zeros((SUB, LANES), jnp.float32)
        for f in range(fields):
            ref, k, base = place(f)
            sums = [ref[k, spot(r + base, 0, t), :] for t in (0, last)]
            for b in range(1, blocks):
                sums = [x + ref[k, spot(r + base, b, t), :] for x, t in zip(sums, (0, last))]
            value = jnp.where(mine[f], pack(jnp.where(low, sums[0], sums[1]), f), value)
        size = SUB // 2
        while size:
            value = value + pltpu.roll(value, size, 0)
            size //= 2
        M[pl.ds(r, 1), :] = value[0:1] * (1.0 / cells)
        return carry

    lax.fori_loop(0, rows, cell_mean, 0, unroll=4)
    peers = nphi - 1 + jnp.where(row > 0, 1, 0) + jnp.where(row < nrow - 1, 1, 0)
    pl.semaphore_wait(barrier, peers)
    for step in range(1, nphi):
        mean_copy(step).start()
    for k in range(EARLY):
        pack_halo(k)
        for c in phi_copies(k):
            c.start()

    index = lax.broadcasted_iota(jnp.int32, (SUB, LANES), 0)

    def local_average(r, carry):
        totals = [polar_cells(r, b) for b in range(blocks)]
        results = list(totals)
        size = 1
        while size < cells:
            if size < SUB:
                turned = []
                for v in totals:
                    forward = pltpu.roll(v, SUB - size, 0)
                    if 2 * size < SUB:
                        forward = jnp.where((index & size) == 0, forward, pltpu.roll(v, size, 0))
                    turned.append(v + forward)
                totals = turned
            else:
                hop = size // SUB
                totals = [totals[b] + totals[b ^ hop] for b in range(blocks)]
            size *= 2
            results = [jnp.where(width == size, v * (1.0 / size), old) for v, old in zip(totals, results)]
        for b in range(blocks):
            Q[pl.ds(pl.multiple_of(r * cells + b * SUB, SUB), SUB), :] = results[b]
        ELO[pl.ds(r, 1), :] = results[0][0:1]
        EHI[pl.ds(r, 1), :] = results[blocks - 1][SUB - 1 : SUB]
        return carry

    lax.fori_loop(0, rows, local_average, 0, unroll=2)

    edge_left = pltpu.make_async_remote_copy(
        src_ref=ELO, dst_ref=ER, send_sem=send_phi.at[0, nvar], recv_sem=recv_phi.at[0, nvar],
        device_id={"phi": left}, device_id_type=MESH)
    edge_right = pltpu.make_async_remote_copy(
        src_ref=EHI, dst_ref=EL, send_sem=send_phi.at[1, nvar], recv_sem=recv_phi.at[1, nvar],
        device_id={"phi": right}, device_id_type=MESH)
    face_left = pltpu.make_async_remote_copy(
        src_ref=SF, dst_ref=RF, send_sem=send_phi.at[0, nvar + 1], recv_sem=recv_phi.at[0, nvar + 1],
        device_id={"phi": left}, device_id_type=MESH)
    edge_left.start()
    edge_right.start()
    for t in range(tiles):
        SF[t] = F[nface - 1, layer(0, 0, t), :]
    for k in range(EARLY, nvar):
        pack_halo(k)
    for k in range(EARLY, nvar):
        for c in phi_copies(k):
            c.start()
    face_left.start()

    MG[phi] = M[...]
    for step in range(1, nphi):
        mean_copy(step).wait_recv()

    def group_mean(who, initial):
        result = initial
        size = 2
        while size <= nphi:
            start = (who // size) * size
            total = MG[start]
            for i in range(1, size):
                total = total + MG[start + i]
            result = jnp.where(width == size * cells, total * (1.0 / size), result)
            size *= 2
        return result

    own_mean = group_mean(phi, M[...])
    next_lo = group_mean(right, jnp.zeros_like(own_mean))
    next_hi = group_mean(left, jnp.zeros_like(own_mean))
    MG[phi] = own_mean
    wide = width > cells

    def spread(r):
        mean = jnp.broadcast_to(MG[phi, pl.ds(r, 1), :], (SUB, LANES))
        for b in range(blocks):
            where = pl.ds(r * cells + b * SUB if isinstance(r, int) else pl.multiple_of(r * cells + b * SUB, SUB), SUB)
            value = jnp.where(wide, mean, Q[where, :])
            for f in range(fields):
                ref, k, base = place(f)
                polar = unpack(value, f)
                ref[k, spot(r + base, b, 0), :] = jnp.where(low, polar, ref[k, spot(r + base, b, 0), :])
                ref[k, spot(r + base, b, last), :] = jnp.where(high, polar, ref[k, spot(r + base, b, last), :])

    for r in (0, 1, rows - 2, rows - 1):
        spread(r)
    lax.fori_loop(2, rows - 2, lambda r, c: (spread(r), c)[1], 0, unroll=4)

    down = pltpu.make_async_remote_copy(
        src_ref=H.at[:, pl.ds(2 * ring, 2 * ring)], dst_ref=H.at[:, pl.ds((rows + 2) * ring, 2 * ring)],
        send_sem=send_row.at[0], recv_sem=recv_row.at[0], device_id={"row": row - 1}, device_id_type=MESH)
    down_face = pltpu.make_async_remote_copy(
        src_ref=F.at[0, pl.ds(0, ring)], dst_ref=FN,
        send_sem=send_row.at[1], recv_sem=recv_row.at[1], device_id={"row": row - 1}, device_id_type=MESH)
    up = pltpu.make_async_remote_copy(
        src_ref=H.at[:, pl.ds(rows * ring, 2 * ring)], dst_ref=H.at[:, pl.ds(0, 2 * ring)],
        send_sem=send_row.at[2], recv_sem=recv_row.at[2], device_id={"row": row + 1}, device_id_type=MESH)

    @pl.when(row > 0)
    def _():
        down.start()
        down_face.start()

    @pl.when(row < nrow - 1)
    def _():
        up.start()

    @pl.when(row == 0)
    def _():
        H[:, pl.ds(0, 2 * ring), :] = jnp.zeros((nvar, 2 * ring, LANES), jnp.float32)

    @pl.when(row == nrow - 1)
    def _():
        H[:, pl.ds((rows + 2) * ring, 2 * ring), :] = jnp.zeros((nvar, 2 * ring, LANES), jnp.float32)
        FN[...] = jnp.zeros_like(FN)

    def whole(ref, k, r, t):
        return jnp.concatenate([ref[k, spot(r, b, t), :] for b in range(blocks)], 0)

    def write(k, r, t, value):
        for b in range(blocks):
            O[k, spot(r, b, t), :] = value[b * SUB : (b + 1) * SUB]

    def shifted(parts, amount):
        out = []
        turned = [pltpu.roll(p, (-amount) % LANES, 1) for p in parts]
        for t in range(tiles):
            if amount > 0:
                inside = lane < LANES - amount
                other = turned[t + 1] if t + 1 < tiles else 0.0
            else:
                inside = lane >= -amount
                other = turned[t - 1] if t > 0 else 0.0
            out.append(jnp.where(inside, turned[t], other))
        return out

    def smooth_row(r):
        for k in range(nvar):
            mid = [whole(H, k, r + 2, t) for t in range(tiles)]
            one = [a + b for a, b in zip(shifted(mid, 1), shifted(mid, -1))]
            two = [a + b for a, b in zip(shifted(mid, 2), shifted(mid, -2))]
            for t in range(tiles):
                v = mid[t]
                s1 = one[t] + (pltpu.roll(v, 1, 0) + pltpu.roll(v, cells - 1, 0)) + (whole(H, k, r + 1, t) + whole(H, k, r + 3, t))
                s2 = two[t] + (pltpu.roll(v, 2, 0) + pltpu.roll(v, cells - 2, 0)) + (whole(H, k, r, t) + whole(H, k, r + 4, t))
                change = (16.0 * s1 - s2 - 90.0 * v) * (1.0 / 12.0)
                write(k, r, t, v + diffusion[k : k + 1, part(t)] * change)

    def field_row(r, following):
        polar = [whole(F, 1, r, t) for t in range(tiles)]
        polar_next = shifted(polar, 1)
        for t in range(tiles):
            write(nvar, r, t, 0.5 * (whole(F, 0, r, t) + following(t)))
            write(nvar + 1, r, t, 0.5 * (polar[t] + polar_next[t]))
            azimuth = whole(F, 2, r, t)
            write(nvar + 2, r, t, 0.5 * (azimuth + pltpu.roll(azimuth, cells - 1, 0)))

    def inner_row(r, carry):
        field_row(r, lambda t: whole(F, 0, r + 1, t))
        smooth_row(r)
        return carry

    lax.fori_loop(2, rows - 2, inner_row, 0, unroll=2)
    for r in (0, 1, rows - 2):
        field_row(r, lambda t, r=r: whole(F, 0, r + 1, t))

    @pl.when(row > 0)
    def _():
        up.wait_recv()

    @pl.when(row < nrow - 1)
    def _():
        down.wait_recv()
        down_face.wait_recv()

    field_row(rows - 1, lambda t: jnp.concatenate([FN[spot(0, b, t), :] for b in range(blocks)], 0))
    for r in (0, 1, rows - 2, rows - 1):
        smooth_row(r)

    edge_left.wait_recv()
    edge_right.wait_recv()
    local = width <= cells
    from_left = jnp.where(local, EL[...], next_hi)
    from_right = jnp.where(local, ER[...], next_lo)

    def fixed(raw, edge, t):
        if t == 0:
            raw = jnp.where(low, edge, raw)
        if t == last:
            raw = jnp.where(high, edge, raw)
        return raw

    for k in range(nvar):
        for c in phi_copies(k):
            c.wait_recv()
        edge_l = unpack(from_left, k)
        edge_r = unpack(from_right, k)
        for t in range(tiles):
            scale = diffusion[k : k + 1, part(t)] * (1.0 / 12.0)
            l1 = fixed(PL[k, 1, t], edge_l, t) - H[k, layer(2, cells - 1, t), :]
            l2 = fixed(PL[k, 0, t], edge_l, t) - H[k, layer(2, cells - 2, t), :]
            r1 = fixed(PR[k, 0, t], edge_r, t) - H[k, layer(2, 0, t), :]
            r2 = fixed(PR[k, 1, t], edge_r, t) - H[k, layer(2, 1, t), :]
            for cell, term in ((0, 16.0 * l1 - l2), (1, -l1), (cells - 2, -r1), (cells - 1, 16.0 * r1 - r2)):
                O[k, layer(0, cell, t), :] = O[k, layer(0, cell, t), :] + scale * term

    face_left.wait_recv()
    edge_f = unpack(from_right, fields - 1)
    for t in range(tiles):
        O[fields - 1, layer(0, cells - 1, t), :] = 0.5 * (F[nface - 1, layer(0, cells - 1, t), :] + fixed(RF[t], edge_f, t))

    for k in range(nvar):
        for c in phi_copies(k):
            c.wait_send()
    edge_left.wait_send()
    edge_right.wait_send()
    face_left.wait_send()
    for step in range(1, nphi):
        mean_copy(step).wait_send()

    @pl.when(row > 0)
    def _():
        down.wait_send()
        down_face.wait_send()

    @pl.when(row < nrow - 1)
    def _():
        up.wait_send()


def spill(pieces, conserved, faces, conserved_out, faces_out, sem):
    fields = conserved.shape[0]
    size = conserved.shape[1] // pieces
    copies = []
    for k in range(fields + faces.shape[0]):
        source, target, i = (conserved, conserved_out, k) if k < fields else (faces, faces_out, k - fields)
        for p in range(pieces):
            where = pl.ds(p * size, size)
            copies.append(pltpu.make_async_copy(source.at[i, where], target.at[i, where], sem.at[k, p]))
    for c in copies:
        c.start()
    for c in copies:
        c.wait()


def blocked(x):
    n, rows, cells, theta = x.shape
    x = x.reshape(n, rows, cells // SUB, SUB, theta // LANES, LANES)
    return x.transpose(0, 1, 2, 4, 3, 5).reshape(n, rows * cells * (theta // LANES), LANES)


def unblocked(x, rows, cells, theta):
    x = x.reshape(x.shape[0], rows, cells // SUB, theta // LANES, SUB, LANES)
    return x.transpose(0, 1, 2, 4, 3, 5).reshape(x.shape[0], rows, cells, theta)


def body(nrow, nphi, hydro_vars, face_b, widths, diffusion):
    nvar, rows, cells, theta = hydro_vars.shape
    nface = face_b.shape[0]
    fields = nvar + nface
    cycles = widths.shape[0] // 2
    tiles = theta // LANES
    ring = cells * tiles
    f32 = jnp.float32
    shape = lambda *s: pltpu.VMEM(s, f32)
    far = pl.BlockSpec(memory_space=pltpu.HBM)
    near = pl.BlockSpec(memory_space=pltpu.VMEM)
    result_bytes = (fields + nface) * rows * ring * LANES * 4
    conserved, faces = pl.pallas_call(
        functools.partial(kernel, nrow, nphi, rows, cells, tiles, cycles),
        out_shape=(
            pltpu.VMEM((fields, rows * ring, LANES), f32),
            pltpu.VMEM((nface, rows * ring, LANES), f32),
        ),
        in_specs=[far, far, far, far],
        out_specs=(near, near),
        scratch_shapes=[
            shape(nvar, (rows + 4) * ring, LANES),
            shape(nvar, 2, tiles, rows, LANES),
            shape(nvar, 2, tiles, rows, LANES),
            shape(nvar, 2, tiles, rows, LANES),
            shape(nvar, 2, tiles, rows, LANES),
            shape(tiles, rows, LANES),
            shape(tiles, rows, LANES),
            shape(ring, LANES),
            shape(rows * cells, LANES),
            shape(rows, LANES),
            shape(nphi, rows, LANES),
            shape(rows, LANES),
            shape(rows, LANES),
            shape(rows, LANES),
            shape(rows, LANES),
            pltpu.SMEM((2 * cycles,), jnp.int32),
            shape(nvar, theta),
            pltpu.SemaphoreType.DMA((2,)),
            pltpu.SemaphoreType.DMA((fields,)),
            pltpu.SemaphoreType.DMA((2, nvar + 2)),
            pltpu.SemaphoreType.DMA((2, nvar + 2)),
            pltpu.SemaphoreType.DMA((nphi,)),
            pltpu.SemaphoreType.DMA((nphi,)),
            pltpu.SemaphoreType.DMA((3,)),
            pltpu.SemaphoreType.DMA((3,)),
        ],
        compiler_params=pltpu.CompilerParams(
            collective_id=0, has_side_effects=True, vmem_limit_bytes=LIMIT - result_bytes
        ),
        name="step",
    )(widths, blocked(hydro_vars), blocked(face_b), diffusion)
    pieces = 2
    conserved, faces = pl.pallas_call(
        functools.partial(spill, pieces),
        out_shape=(
            jax.ShapeDtypeStruct((fields, rows * ring, LANES), f32),
            jax.ShapeDtypeStruct((nface, rows * ring, LANES), f32),
        ),
        in_specs=[near, near],
        out_specs=(far, far),
        scratch_shapes=[pltpu.SemaphoreType.DMA((fields + nface, pieces))],
        compiler_params=pltpu.CompilerParams(vmem_limit_bytes=1000000),
        name="spill",
    )(conserved, faces)
    return unblocked(conserved, rows, cells, theta), unblocked(faces, rows, cells, theta)


def solution(mesh):
    spec = P(None, "row", "phi", None)
    return jax.shard_map(
        functools.partial(body, mesh.shape["row"], mesh.shape["phi"]),
        mesh=mesh,
        in_specs=(spec, spec, P(), P()),
        out_specs=(spec, spec),
        check_vma=False,
    )
```
